128 devices in a mesh: sub: 8 (over x_hi, y), clu: 16 (over z, x_lo, core).
Axes of the slice: x: 4 (x_hi: 2, x_lo: 2; x = x_hi * 2 + x_lo), y: 4, z: 4, core: 2. Of those that a mesh axis runs over, the one named last changes fastest.
Arguments:
- right_side: float32 [262144, 256], P(('sub', 'clu')), may hold values from -6 to 6
- near_blocks: float32 [512, 3, 512, 512], P(('sub', 'clu')), may hold values from -0.15625 to 0.15625
- near_index: int32 [512, 3], P(('sub', 'clu')), may hold values from 0 to 511, as said below
- bases: float32 [512, 512, 128], P(('sub', 'clu')), may hold values from -0.25 to 0.25
- leaf_transfer: float32 [512, 128, 128], P(('sub', 'clu')), may hold values from -0.25 to 0.25
- cluster_transfer: float32 [128, 128, 128], P(('sub', 'clu')), may hold values from -0.125 to 0.125
- cluster_coupling: float32 [128, 4, 128, 128], P(('sub', 'clu')), may hold values from -0.25 to 0.25
- cluster_list: int32 [128, 4], P(('sub', 'clu')), may hold values from 0 to 127, as said below
- subtree_coupling: float32 [8, 3, 128, 128], P('sub'), may hold values from -0.3125 to 0.3125
- subtree_list: int32 [8, 3], P('sub'), may hold values from 0 to 7, as said below
Outputs:
- solution: float32 [262144, 256], P(('sub', 'clu'))
- residual: float32 [262144, 256], P(('sub', 'clu'))
The draws below stay inside these ranges and needn't reach their ends.
Inputs may be any that keep to these rules, and one draw needn't show every extreme that they name: `near_index`: row g begins with g itself; its other entries are two different leaves within 2 leaves of g held by the same subtree; the first leaf of a cluster names the leaf before it, and the last the leaf after it, where those lie in the same subtree. `cluster_list`: the entries of a row are different clusters of the same subtree as the row's cluster, never that cluster itself. `subtree_list`: the entries of a row are different subtrees, never the row's own.
All inputs are finite; a program needn't handle non-finite values.
Results may differ from the reference program's by a relative error of at most 0.0001.
Values sent between devices are 32-bit elements; how exact they have to be, the bound alone decides.
No kernel may reach another device: no remote copies, remote signals or barrier semaphores. Data moves between devices by JAX's collectives and lax.ppermute only.
A program may use at most 128 MiB of HBM per device.

```python
import jax
import jax.numpy as jnp
from jax import lax

LEAF = 512
RANK = 128
RHS = 256
NEAR = 3
NCC = 4
NSC = 3
ITERS = 3
LEAF_DEV = 4
CLUSTERS = 128
SUBTREES = 8
LEAVES = 512
ROWS = 262144


def draw_near_index(key, part):
    leaf_ids = jnp.arange(LEAVES, dtype=jnp.int32)
    offsets = jnp.array([-2, -1, 1, 2], dtype=jnp.int32)
    targets = leaf_ids[:, None] + offsets[None, :]
    span = LEAF_DEV * (CLUSTERS // SUBTREES)
    valid = (targets >= 0) & (targets < LEAVES) & (targets // span == leaf_ids[:, None] // span)
    scores = jax.random.randint(key, (LEAVES, 4), 0, 1000, dtype=jnp.int32) * 8 + jnp.arange(4, dtype=jnp.int32)[None, :]
    position = leaf_ids % LEAF_DEV
    forced = (position[:, None] == 0) & (offsets[None, :] == -1) | (position[:, None] == LEAF_DEV - 1) & (offsets[None, :] == 1)
    scores = scores + jnp.where(forced, 100000, 0)
    scores = jnp.where(valid, scores, -10000000)
    order = jnp.argsort(-scores, axis=1, stable=True)[:, :2]
    chosen = jnp.take_along_axis(targets, order, axis=1)
    return jnp.concatenate([leaf_ids[:, None], chosen], axis=1).astype(jnp.int32)


def draw_cluster_list(key, part):
    per_subtree = CLUSTERS // SUBTREES
    cluster_ids = jnp.arange(CLUSTERS, dtype=jnp.int32)
    local_ids = jnp.arange(per_subtree, dtype=jnp.int32)
    scores = jax.random.randint(jax.random.fold_in(key, 7), (CLUSTERS, per_subtree), 0, 1000, dtype=jnp.int32) * per_subtree + local_ids[None, :]
    scores = jnp.where(local_ids[None, :] == (cluster_ids % per_subtree)[:, None], -1000000, scores)
    order = jnp.argsort(-scores, axis=1, stable=True)[:, :NCC].astype(jnp.int32)
    return ((cluster_ids // per_subtree)[:, None] * per_subtree + order).astype(jnp.int32)


def draw_subtree_list(key, part):
    subtree_ids = jnp.arange(SUBTREES, dtype=jnp.int32)
    scores = jax.random.randint(jax.random.fold_in(key, 11), (SUBTREES, SUBTREES), 0, 1000, dtype=jnp.int32) * SUBTREES + subtree_ids[None, :]
    scores = jnp.where(subtree_ids[None, :] == subtree_ids[:, None], -1000000, scores)
    return jnp.argsort(-scores, axis=1, stable=True)[:, :NSC].astype(jnp.int32)


def levels(key, extent, cuts, smallest, high):
    loudness = 1.0
    for axis_at, shards_of in cuts:
        steps = jax.random.uniform(jax.random.fold_in(jax.random.fold_in(key, 6), axis_at), (shards_of,), jnp.float32, smallest / len(cuts), high / len(cuts))
        loudness = loudness * jnp.repeat(jnp.exp(steps), extent[axis_at] // shards_of).reshape((-1,) + (1,) * (len(extent) - 1 - axis_at))
    return loudness


def bell_draw(stream_key, extent, scale, most, shards=(), held_as=jnp.bfloat16):
    factor_of = levels(stream_key, extent, shards, -0.22, 0.18) if shards else 1.0
    values = jax.random.normal(stream_key, extent, jnp.float32) * scale * factor_of
    return jnp.minimum(jnp.maximum(values, -most), most).astype(held_as)


def setup_inputs(seed: int = 0) -> dict:
    splits = jax.random.split(jax.random.key(seed), 11)
    return {
        "right_side": bell_draw(splits[0], (ROWS, RHS), 1.0, 6.0, ((0, 128),), jnp.float32),
        "near_blocks": bell_draw(splits[1], (LEAVES, NEAR, LEAF, LEAF), (LEAF * NEAR) ** -0.5, 0.15625, ((0, 128),), jnp.float32),
        "near_index": draw_near_index(jax.random.fold_in(splits[10], 71), 0),
        "bases": bell_draw(splits[3], (LEAVES, LEAF, RANK), LEAF ** -0.5, 0.25, ((0, 128),), jnp.float32),
        "leaf_transfer": bell_draw(splits[4], (LEAVES, RANK, RANK), (RANK * LEAF_DEV) ** -0.5, 0.25, ((0, 128),), jnp.float32),
        "cluster_transfer": bell_draw(splits[5], (CLUSTERS, RANK, RANK), (RANK * CLUSTERS // SUBTREES) ** -0.5, 0.125, ((0, 128),), jnp.float32),
        "cluster_coupling": bell_draw(splits[6], (CLUSTERS, NCC, RANK, RANK), (RANK * NCC) ** -0.5, 0.25, ((0, 128),), jnp.float32),
        "cluster_list": draw_cluster_list(jax.random.fold_in(splits[10], 71), 0),
        "subtree_coupling": bell_draw(splits[8], (SUBTREES, NSC, RANK, RANK), (RANK * NSC) ** -0.5, 0.3125, ((0, 8),), jnp.float32),
        "subtree_list": draw_subtree_list(jax.random.fold_in(splits[10], 71), 0),
    }


highest = lax.Precision.HIGHEST
spectrum_center = 3.0
spectrum_radius = 2.0
ridge_shift = 3.0


def near_field(vector_in, near_blocks, near_index):
    leaves = vector_in.reshape(LEAVES, LEAF, RHS)

    def one_leaf(pair):
        blocks, picks = pair
        return jnp.einsum('jab,jbr->ar', blocks, leaves[picks], precision=highest)

    return lax.map(one_leaf, (near_blocks, near_index)).reshape(ROWS, RHS)


def far_field(vector_in, bases, leaf_transfer, cluster_transfer, cluster_coupling, cluster_list, subtree_coupling, subtree_list):
    per_subtree = CLUSTERS // SUBTREES
    leaves = vector_in.reshape(LEAVES, LEAF, RHS)
    leaf_coeffs = jnp.einsum('lak,lar->lkr', bases, leaves, precision=highest)
    grouped = leaf_coeffs.reshape(CLUSTERS, LEAF_DEV, RANK, RHS)
    transfers = leaf_transfer.reshape(CLUSTERS, LEAF_DEV, RANK, RANK)
    cluster_coeffs = jnp.einsum('dlkm,dlkr->dmr', transfers, grouped, precision=highest)
    upper = cluster_transfer.reshape(SUBTREES, per_subtree, RANK, RANK)
    subtree_coeffs = jnp.einsum('scka,sckr->sar', upper, cluster_coeffs.reshape(SUBTREES, per_subtree, RANK, RHS), precision=highest)
    cluster_far = jnp.einsum('djab,djbr->dar', cluster_coupling, cluster_coeffs[cluster_list], precision=highest)
    subtree_far = jnp.einsum('sjab,sjbr->sar', subtree_coupling, subtree_coeffs[subtree_list], precision=highest)
    spread = jnp.einsum('scka,sar->sckr', upper, subtree_far, precision=highest).reshape(CLUSTERS, RANK, RHS)
    combined = cluster_far + spread
    lowered = jnp.einsum('dlkm,dmr->dlkr', transfers, combined, precision=highest).reshape(LEAVES, RANK, RHS)
    return jnp.einsum('lak,lkr->lar', bases, lowered, precision=highest).reshape(ROWS, RHS)


def reference(right_side, near_blocks, near_index, bases, leaf_transfer, cluster_transfer, cluster_coupling, cluster_list, subtree_coupling, subtree_list):
    def operator(vector_in):
        near = near_field(vector_in, near_blocks, near_index)
        far = far_field(vector_in, bases, leaf_transfer, cluster_transfer, cluster_coupling, cluster_list, subtree_coupling, subtree_list)
        return ridge_shift * vector_in + near + far

    solution = jnp.zeros_like(right_side)
    residual = right_side
    update = right_side / spectrum_center
    weight_old = spectrum_radius / spectrum_center
    for turn_index in range(ITERS):
        solution = solution + update
        residual = residual - operator(update)
        if turn_index + 1 < ITERS:
            weight_new = 1.0 / (2.0 * spectrum_center / spectrum_radius - weight_old)
            update = (weight_new * weight_old) * update + (2.0 * weight_new / spectrum_radius) * residual
            weight_old = weight_new
    return solution, residual
```

```python
import jax
import jax.numpy as jnp
from jax import lax
from jax.experimental import pallas as pl
from jax.experimental.pallas import tpu as pltpu
from jax.sharding import PartitionSpec as P

REACH = 2
ITERS = 3
spectrum_center = 3.0
spectrum_radius = 2.0
ridge_shift = 3.0

f32 = jnp.float32
bf16 = jnp.bfloat16


def split(value):
    high = value.astype(bf16)
    return high, (value - high.astype(f32)).astype(bf16)


def dot3(a, b, dims=((1,), (0,))):
    a_high, a_low = a if isinstance(a, tuple) else split(a)
    b_high, b_low = b if isinstance(b, tuple) else split(b)

    def one(x, y):
        return lax.dot_general(x, y, (dims, ((), ())), preferred_element_type=f32)

    return one(a_high, b_high) + (one(a_high, b_low) + one(a_low, b_high))


def call(kernel, ins, args, outs, scratch=(), flops=0):
    return pl.pallas_call(
        kernel,
        in_specs=ins,
        out_specs=[VMEM] * len(outs),
        out_shape=[jax.ShapeDtypeStruct(shape, kind) for shape, kind in outs],
        scratch_shapes=list(scratch),
        compiler_params=pltpu.CompilerParams(vmem_limit_bytes=LIMIT),
        cost_estimate=pl.CostEstimate(flops=flops, transcendentals=0, bytes_accessed=0) if flops else None,
    )(*args)


LIMIT = 36 * 1024 * 1024
VMEM = pl.BlockSpec(memory_space=pltpu.VMEM)
SMEM = pl.BlockSpec(memory_space=pltpu.SMEM)
HBM = pl.BlockSpec(memory_space=pltpu.HBM)


def dot(a, b, dims=((1,), (0,))):
    return lax.dot_general(a, b, (dims, ((), ())), preferred_element_type=f32)


def gather_coeffs(wt, value):
    rank = wt.shape[0] // 2
    high, low = split(value)
    both = dot(wt, high)
    return both[:rank] + (both[rank:] + dot(wt[:rank], low))


def setup_kernel(bases, transfer, right, upper, w_out, wt_out, c_out, p_out):
    count, _, _ = bases.shape

    def leaf(at, total):
        folded = dot3(bases[at], transfer[at])
        high, low = split(folded)
        w_out[at] = jnp.concatenate([high, low], axis=1)
        high, low = split(folded.T)
        wt_out[at] = jnp.concatenate([high, low], axis=0)
        return total + gather_coeffs(wt_out[at], right[at] * (1.0 / spectrum_center))

    total = lax.fori_loop(0, count, leaf, jnp.zeros(c_out.shape, f32))
    c_out[...] = total
    p_out[...] = dot3(total, upper[...], ((0,), (0,)))


def fold_setup(bases, transfer, right, upper):
    count, rows, rank = bases.shape
    columns = right.shape[-1]
    return call(
        setup_kernel,
        [VMEM] * 4,
        [bases, transfer, right, upper],
        [
            ((count, rows, 2 * rank), bf16),
            ((count, 2 * rank, rows), bf16),
            ((rank, columns), f32),
            ((columns, rank), f32),
        ],
    )


def local(near, device, leaf, j, leaves):
    return near[leaf, j] - device[0] * leaves


def near_own(scale, first, last, device, near, blocks, update, residual, right=None, older=None):
    leaves, _, _ = update.shape

    def kernel(device, near, blocks, update, *rest):
        if last:
            residual, right, older, out, total, held, high, low, sems = rest
        elif first:
            out, held, high, low, sems = rest
        else:
            residual, out, held, high, low, sems = rest

        def own(leaf, j):
            at = local(near, device, leaf, j, leaves)
            return at, (at >= 0) & (at < leaves)

        def copy(leaf, j):
            at = leaf * 3 + j
            return pltpu.make_async_copy(blocks.at[at], held.at[at], sems.at[at])

        def start(leaf, _):
            copy(leaf, 0).start()
            for j in (1, 2):
                pl.when(own(leaf, j)[1])(lambda j=j: copy(leaf, j).start())
            return 0

        lax.fori_loop(0, leaves, start, 0)

        def halve(leaf, _):
            value = update[leaf] * scale if first else update[leaf]
            high[leaf], low[leaf] = split(value)
            return 0

        lax.fori_loop(0, leaves, halve, 0)

        def product(leaf, j, at):
            return dot3(held[leaf * 3 + j], (high[at], low[at]))

        def each(leaf, _):
            copy(leaf, 0).wait()
            value = update[leaf] * scale if first else update[leaf]
            begin = update[leaf] if first else residual[leaf]
            out[leaf] = begin - ridge_shift * value - product(leaf, 0, leaf)
            if last:
                total[leaf] = right[leaf] * (1.0 / spectrum_center) + older[leaf] + value
            for j in (1, 2):
                at, here = own(leaf, j)

                @pl.when(here)
                def _():
                    copy(leaf, j).wait()
                    out[leaf] -= product(leaf, j, jnp.clip(at, 0, leaves - 1))

            return 0

        lax.fori_loop(0, leaves, each, 0)

    args = [device, near, blocks, update]
    if not first:
        args.append(residual)
    if last:
        args += [right, older]
    return call(
        kernel,
        [SMEM, SMEM, HBM] + [VMEM] * (len(args) - 3),
        args,
        [(update.shape, f32)] * (2 if last else 1),
        [
            pltpu.VMEM(blocks.shape, f32),
            pltpu.VMEM(update.shape, bf16),
            pltpu.VMEM(update.shape, bf16),
            pltpu.SemaphoreType.DMA((blocks.shape[0],)),
        ],
        flops=4_000_000_000,
    )


def finish(scale, keep, gain, last, device, near, clusters, blocks, low, high, partial, update, w, wt, near_c, far_c, coupling, upper, lifted):
    leaves, rows, columns = partial.shape
    rank = upper.shape[0]

    def kernel(device, near, clusters, blocks, low, high, partial, *rest):
        if last:
            w, near_c, far_c, coupling, upper, f0, f1, f2, f3, out, held, turned, sems = rest
        else:
            (update, w, wt, near_c, far_c, coupling, upper, f0, f1, f2, f3, out, u_out, c_out, p_out) = rest[:15]
            held, turned, sems = rest[15:]
        clu = device[0] & 15
        z, x, core = clu >> 2, (clu >> 1) & 1, clu & 1

        def other(leaf, j):
            at = local(near, device, leaf, j, leaves)
            return at, (at < 0) | (at >= leaves)

        def copy(leaf, j):
            slot = leaf * 2 + j - 1
            return pltpu.make_async_copy(blocks.at[leaf * 3 + j], held.at[slot], sems.at[slot])

        def start(leaf, _):
            for j in (1, 2):
                pl.when(other(leaf, j)[1])(lambda j=j: copy(leaf, j).start())
            return 0

        lax.fori_loop(0, leaves, start, 0)
        for k, piece in enumerate((f0, f1, f2, f3)):
            turned[(z - k) & 3] = piece[...]
        down = dot3(upper[...], turned[...].reshape(columns, rank), ((1,), (1,)))
        for k in range(coupling.shape[0]):
            listed = clusters[0, k] & 15
            there = ((z - (listed >> 2)) & 3) * 2 + (((listed >> 1) & 1) ^ x)
            coeffs = jnp.where((listed & 1) == core, near_c[there], far_c[there])
            down += dot3(coupling[k], coeffs)
        down_high, down_low = split(down)
        down_twice = jnp.concatenate([down_high, down_high], axis=0)

        def each(leaf, total):
            out[leaf] = partial[leaf] - (dot(w[leaf], down_twice) + dot(w[leaf, :, :rank], down_low))
            for j in (1, 2):
                at, there = other(leaf, j)

                @pl.when(there)
                def _():
                    copy(leaf, j).wait()
                    below = low[jnp.clip(at + REACH, 0, REACH - 1)]
                    above = high[jnp.clip(at - leaves, 0, REACH - 1)]
                    value = jnp.where(at < 0, below, above)
                    out[leaf] -= dot3(held[leaf * 2 + j - 1], value * scale if scale != 1.0 else value)

            if last:
                return total
            renewed = (keep * scale) * update[leaf] + gain * out[leaf]
            u_out[leaf] = renewed
            return total + gather_coeffs(wt[leaf], renewed)

        if last:
            lax.fori_loop(0, leaves, each, 0)
        else:
            total = lax.fori_loop(0, leaves, each, jnp.zeros((rank, columns), f32))
            c_out[...] = total
            p_out[...] = dot3(total, upper[...], ((0,), (0,)))

    args = [device, near, clusters, blocks, low, high, partial]
    args += [w] if last else [update, w, wt]
    args += [near_c, far_c, coupling, upper, *lifted]
    outs = [(partial.shape, f32)]
    if not last:
        outs += [(partial.shape, f32), ((rank, columns), f32), ((columns, rank), f32)]
    return call(
        kernel,
        [SMEM, SMEM, SMEM, HBM] + [VMEM] * (len(args) - 4),
        args,
        outs,
        [
            pltpu.VMEM((2 * leaves, rows, rows), f32),
            pltpu.VMEM((4, columns // 4, rank), f32),
            pltpu.SemaphoreType.DMA((2 * leaves,)),
        ],
        flops=3_000_000_000,
    )


def pair_kernel(p, c, upper, out):
    out[...] = p[...] + dot3(c[...], upper[...], ((0,), (0,)))


def pair_sum(p, c, upper):
    return call(pair_kernel, [VMEM] * 3, [p, c, upper], [(p.shape, f32)])[0]


def quarters(device, q, other):
    piece = q.shape[0] // 4

    def kernel(device, q, other, *outs):
        z = (device[0] & 15) >> 2
        for k, out in enumerate(outs):
            rows = pl.ds(((z + k) & 3) * piece, piece)
            out[...] = q[rows] + other[rows]

    return call(kernel, [SMEM, VMEM, VMEM], [device, q, other], [((piece, q.shape[1]), f32)] * 4)


def subtree_far(device, listed, pieces, coupling):
    def kernel(device, listed, g0, g1, g2, g3, coupling, out, held):
        sub = device[0] >> 4
        for k, piece in enumerate((g0, g1, g2, g3)):
            held[2 * k] = piece[0]
            held[2 * k + 1] = piece[1]
        total = None
        for k in range(coupling.shape[0]):
            there = listed[0, k]
            at = ((sub - there) & 3) * 2 + ((sub ^ there) >> 2)
            part = dot3(held[at], coupling[k], ((1,), (1,)))
            total = part if total is None else total + part
        out[...] = total

    shape = pieces[0].shape[1:]
    return call(
        kernel,
        [SMEM, SMEM] + [VMEM] * 5,
        [device, listed, *pieces, coupling],
        [(shape, f32)],
        [pltpu.VMEM((8, *shape), f32)],
    )[0]


def after(value, *others):
    return lax.optimization_barrier((value, *others))[0]


def body(
    right_side,
    near_blocks,
    near_index,
    bases,
    leaf_transfer,
    cluster_transfer,
    cluster_coupling,
    cluster_list,
    subtree_coupling,
    subtree_list,
):
    leaves, rows = bases.shape[:2]
    columns = right_side.shape[1]
    clu_count, sub_count = lax.axis_size("clu"), lax.axis_size("sub")
    device = (lax.axis_index("sub") * clu_count + lax.axis_index("clu")).astype(jnp.int32).reshape(1)

    def clu_swap(value, bits):
        return lax.ppermute(value, "clu", [(i, i ^ bits) for i in range(clu_count)])

    def z_shift(value, by):
        return lax.ppermute(value, "clu", [(i, (i + 4 * by) % clu_count) for i in range(clu_count)])

    def y_shift(value, by):
        return lax.ppermute(value, "sub", [(i, (i & 4) + (i + by) % 4) for i in range(sub_count)])

    def diagonal(value):
        pairs = [
            (s * clu_count + i, (s ^ 4) * clu_count + (i ^ 2)) for s in range(sub_count) for i in range(clu_count)
        ]
        return lax.ppermute(value, ("sub", "clu"), pairs)

    forward = [(i, i + 1) for i in range(clu_count - 1)]
    backward = [(i + 1, i) for i in range(clu_count - 1)]

    blocks = near_blocks.reshape(leaves * 3, rows, rows)
    right = right_side.reshape(leaves, rows, columns)
    upper = cluster_transfer[0]
    upper_x = clu_swap(upper, 2)
    w, wt, coeffs, lifted = fold_setup(bases, leaf_transfer, right, upper)

    update, residual, older = right, None, None
    weight_old = spectrum_radius / spectrum_center
    for turn in range(ITERS):
        first, last = turn == 0, turn + 1 == ITERS
        scale = 1.0 / spectrum_center if first else 1.0
        coeffs_x = clu_swap(coeffs, 2)
        sent = after(update, coeffs_x)
        low = lax.ppermute(sent[leaves - REACH :], "clu", forward)
        high = lax.ppermute(sent[:REACH], "clu", backward)
        q = pair_sum(lifted, coeffs_x, upper_x)
        q_other = clu_swap(q, 1)
        pieces = quarters(device, q, q_other)
        q = pieces[0]
        for by in (1, 2, 3):
            q = q + z_shift(pieces[by], by)
        q = jnp.stack([q, diagonal(q)])
        subtrees = [q]
        for by in (1, 2, 3):
            subtrees.append(y_shift(q, by))
        lifted_far = [subtree_far(device, subtree_list, subtrees, subtree_coupling[0])]
        for by in (1, 2, 3):
            lifted_far.append(z_shift(lifted_far[0], by))
        pair = after(jnp.stack([coeffs, coeffs_x]), pieces[0])
        near_c = [pair]
        for by in (1, 2, 3):
            near_c.append(z_shift(pair, by))
        near_c = jnp.concatenate(near_c)
        far_c = clu_swap(near_c, 1)
        mine = after(update, lifted_far[0])
        if last:
            partial, solution = near_own(scale, first, last, device, near_index, blocks, mine, residual, right, older)
        else:
            (partial,) = near_own(scale, first, last, device, near_index, blocks, mine, residual)
        weight_new = 1.0 / (2.0 * spectrum_center / spectrum_radius - weight_old)
        keep, gain = weight_new * weight_old, 2.0 * weight_new / spectrum_radius
        weight_old = weight_new
        done = finish(
            scale, keep, gain, last, device, near_index, cluster_list, blocks, low, high, partial, update, w, wt,
            near_c, far_c, cluster_coupling[0], upper, lifted_far,
        )
        if last:
            residual = done[0]
        else:
            older = update
            residual, update, coeffs, lifted = done
    return solution.reshape(right_side.shape), residual.reshape(right_side.shape)


def solution(mesh):
    placed = (
        P(("sub", "clu"), None),
        P(("sub", "clu"), None, None, None),
        P(("sub", "clu"), None),
        P(("sub", "clu"), None, None),
        P(("sub", "clu"), None, None),
        P(("sub", "clu"), None, None),
        P(("sub", "clu"), None, None, None),
        P(("sub", "clu"), None),
        P("sub", None, None, None),
        P("sub", None),
    )
    return jax.shard_map(
        body,
        mesh=mesh,
        in_specs=placed,
        out_specs=(P(("sub", "clu"), None), P(("sub", "clu"), None)),
        check_vma=False,
    )
```
